32 devices in a mesh: groups: 1, expert: 32 (over z, y, x, core), hidden: 1.
Axes of the slice: x: 2, y: 2, z: 4, core: 2. Of those that a mesh axis runs over, the one named last changes fastest.
Arguments:
- tokens: bfloat16 [512, 4096], P(('groups', 'expert')), may hold values from -6 to 6
- expert_ids: int32 [512, 8], P(('groups', 'expert')), may hold values from 0 to 15, all different within a row; in each aligned block of 16 rows (0 to 15, 16 to 31, ...) at most 16 rows name the same one
- router_scores: float32 [512, 8], P(('groups', 'expert')), may hold values from 0.05 to 1
- gate_weight: bfloat16 [32, 4096, 512], P('expert', None, 'hidden'), may hold values from -0.09375 to 0.09375
- up_weight: bfloat16 [32, 4096, 512], P('expert', None, 'hidden'), may hold values from -0.09375 to 0.09375
- down_weight: bfloat16 [32, 512, 4096], P('expert', 'hidden'), may hold values from -0.1875 to 0.1875
Outputs:
- moe_out: bfloat16 [512, 4096], P(('groups', 'expert'), 'hidden')
The draws below stay inside these ranges and needn't reach their ends.
Inputs may be any that keep to these rules, and one draw needn't show every extreme that they name: `expert_ids`: each row names 8 different experts. In each aligned block of 16 rows no expert is named by more than 16 rows, a bound that some block reaches.
All inputs are finite; a program needn't handle non-finite values.
Results may differ from the reference program's by a relative error of at most 0.012.
Values may be sent and summed in bfloat16 or wider, within the bound.
A program may use at most 64 MiB of HBM per device.

```python
import math
import jax
import jax.numpy as jnp
import numpy as np
from jax import lax

D = 4096
HID = 1024
SPAN = 2
TOK_DEV = 16
TOKENS = 512
EXPERTS = 16
SLOTS = 32
TOPK = 8
HS = 512
PIECE = 512
CAP = 16
N_EXPERT = 32


def block_levels(stream_key, shape, pieces, smallest, top_value):
    gain, own = 1.0, jax.random.fold_in(stream_key, 6)
    for dim, shards_of in pieces:
        heights = jnp.exp(jax.random.uniform(jax.random.fold_in(own, dim), (shards_of,), jnp.float32, smallest / len(pieces), top_value / len(pieces)))
        gain = gain * jnp.repeat(heights, shape[dim] // shards_of).reshape([-1 if axis == dim else 1 for axis in range(len(shape))])
    return gain


def deal_out(key, own, number, rows, number_of, top, limit, lean):
    sequence = jax.random.permutation(key, number_of)
    packed, ordinary = shares(number_of, rows * top, limit, lean, True), shares(number_of, rows * top, limit, lean, False)
    places = jnp.arange(number_of)

    def named(tallies, offset_by):
        used = int((tallies > 0).sum())
        fixed = max(1, used // 4)
        moved = fixed + (places - fixed + offset_by * (used - fixed)) % max(1, number_of - fixed)
        return jnp.zeros((number_of,), jnp.int32).at[sequence[jnp.where(places < fixed, places, moved)]].set(jnp.asarray(tallies, jnp.int32))

    tallies = jnp.where(number % 4 == 0, named(packed, number // 4), named(ordinary, number - number // 4 - 1))
    mixed = jax.random.permutation(jax.random.fold_in(own, 3), number_of)
    giver, sink = mixed[0:number_of // 2 * 2:2], mixed[1:number_of // 2 * 2:2]
    margin = jnp.minimum(tallies[giver] - 1, limit - tallies[sink]) // 2
    margin = jnp.where((giver == sequence[0]) | (sink == sequence[0]) | (tallies[sink] == 0), 0, jnp.maximum(margin, 0))
    moved = jax.random.randint(jax.random.fold_in(own, 4), (number_of // 2,), 0, 1 << 20) % (margin + 1)
    tallies = tallies.at[giver].add(-moved).at[sink].add(moved)
    members = jnp.searchsorted(jnp.cumsum(tallies), jnp.arange(rows * top), side="right").astype(jnp.int32)
    listing = members.reshape(top, rows).T
    listing = listing[jax.random.permutation(jax.random.fold_in(own, 1), rows)]
    offset_by = jax.random.randint(jax.random.fold_in(own, 2), (rows, 1), 0, top)
    return jnp.take_along_axis(listing, (jnp.arange(top)[None, :] + offset_by) % top, axis=1)


def shares(amount, total, most, skew, full):
    portions = [(1 << 20) // math.isqrt(rank ** skew) + 1 for rank in range(1, amount + 1)]
    largest = most if full else min(most, max(-(-total // amount), total * portions[0] // sum(portions)))
    least = 1 if total - largest >= amount - 1 else 0
    holding, surplus = [largest] + [least] * (amount - 1), total - largest - least * (amount - 1)
    while surplus > 0:
        movable = [i for i in range(1, amount) if holding[i] < largest] or [i for i in range(1, amount) if holding[i] < most]
        whole, remaining = sum([portions[i] for i in movable]), surplus
        for i in movable:
            addition = min(most - holding[i], max(1, remaining * portions[i] // whole), surplus)
            holding[i] = holding[i] + addition
            surplus = surplus - addition
    return np.array(holding)


def normal_values(own_key, shape, deviation, most, split=(), kind=jnp.bfloat16):
    gain = block_levels(own_key, shape, split, -0.22, 0.18) if split else 1.0
    entries = jax.random.normal(own_key, shape, jnp.float32) * deviation * gain
    return jnp.minimum(jnp.maximum(entries, -most), most).astype(kind)


def setup_inputs(seed: int = 0, part: int = 0) -> dict:
    arg_keys = jax.random.split(jax.random.key(seed), 7)
    part_splits = jax.random.split(jax.random.fold_in(arg_keys[6], part), 7)
    tokens = normal_values(part_splits[0], (TOKENS, D), 1.0, 6.0, ((0, 32),))
    expert_ids_keys = jax.random.split(jax.random.fold_in(part_splits[1], 1), TOKENS // TOK_DEV)
    expert_ids_turns = jax.random.permutation(jax.random.fold_in(part_splits[1], 3), TOKENS // TOK_DEV)
    expert_ids = jax.vmap(lambda own, number: deal_out(jax.random.fold_in(part_splits[1], 2), own, number, TOK_DEV, EXPERTS, TOPK, CAP, 2))(expert_ids_keys, expert_ids_turns).reshape((TOKENS, TOPK))
    router_scores = jnp.clip(jnp.exp(math.log(1.0) - 2.9957323 * jax.random.uniform(part_splits[2], (TOKENS, TOPK), jnp.float32) ** block_levels(part_splits[2], (TOKENS, TOPK), ((0, 32),), -0.2, 0.2)), 0.05, 1.0)
    gate_weight = normal_values(arg_keys[3], (SLOTS, D, HS), D ** -0.5, 0.09375, ((0, 32),))
    up_weight = normal_values(arg_keys[4], (SLOTS, D, HS), D ** -0.5, 0.09375, ((0, 32),))
    down_weight = normal_values(arg_keys[5], (SLOTS, HS, D), HID ** -0.5, 0.1875, ((0, 32),))
    return dict(tokens=tokens, expert_ids=expert_ids, router_scores=router_scores, gate_weight=gate_weight, up_weight=up_weight, down_weight=down_weight)


def routed_weights(router_scores):
    return 2.5 * router_scores / jnp.sum(router_scores, axis=1, keepdims=True)


def positions(pair_ids, expert_count):
    onehot = (pair_ids[:, None] == jnp.arange(expert_count, dtype=jnp.int32)[None, :]).astype(jnp.int32)
    before = jnp.cumsum(onehot, axis=0) - onehot
    return jnp.sum(before * onehot, axis=1).astype(jnp.int32)


def reference(tokens, expert_ids, router_scores, gate_weight, up_weight, down_weight):
    blocks = N_EXPERT
    pair_count = TOK_DEV * TOPK
    pair_ids = expert_ids.reshape(blocks, pair_count).astype(jnp.int32)
    position = jax.vmap(lambda block_ids: positions(block_ids, EXPERTS))(pair_ids)
    slot_index = (pair_ids * CAP + position).astype(jnp.int32)
    local_token = (jnp.arange(pair_count, dtype=jnp.int32) // TOPK).astype(jnp.int32)
    owner_start = jnp.full((blocks, EXPERTS * CAP), TOK_DEV, jnp.int32)
    owner_row = jax.vmap(lambda start_row, slot_row: start_row.at[slot_row].set(local_token))(owner_start, slot_index)
    routed = routed_weights(router_scores).reshape(blocks, pair_count)
    slot_weight = jax.vmap(lambda slot_row, weight_row: jnp.zeros((EXPERTS * CAP,), jnp.float32).at[slot_row].set(weight_row))(slot_index, routed)
    padded = jnp.concatenate([tokens.reshape(blocks, TOK_DEV, D), jnp.zeros((blocks, 1, D), tokens.dtype)], axis=1)
    flat_rows = padded.reshape(blocks * (TOK_DEV + 1), D)
    block_base = (jnp.arange(blocks, dtype=jnp.int32) * (TOK_DEV + 1))[:, None]
    row_table = (block_base + owner_row).astype(jnp.int32).reshape(blocks, EXPERTS, CAP)
    weight_table = slot_weight.reshape(blocks, EXPERTS, CAP)
    gate_slots = gate_weight.reshape(EXPERTS, SPAN, D, HS)
    up_slots = up_weight.reshape(EXPERTS, SPAN, D, HS)
    down_pieces = down_weight.reshape(EXPERTS, HID // PIECE, PIECE, D)

    def one_expert(running, expert):
        row_index = row_table[:, expert, :].reshape(-1)
        weight_col = weight_table[:, expert, :].reshape(-1)
        row_data = flat_rows[row_index]
        gate_full = jnp.transpose(gate_slots[expert], (1, 0, 2)).reshape(D, HID)
        up_full = jnp.transpose(up_slots[expert], (1, 0, 2)).reshape(D, HID)
        gate_val = jnp.dot(row_data, gate_full, preferred_element_type=jnp.float32)
        up_val = jnp.dot(row_data, up_full, preferred_element_type=jnp.float32)
        activated = (jax.nn.silu(gate_val) * up_val).astype(jnp.bfloat16)
        split_act = activated.reshape(-1, HID // PIECE, PIECE).astype(jnp.float32)
        products = jnp.einsum('rgp,gpd->grd', split_act, down_pieces[expert].astype(jnp.float32))
        rounded = lax.optimization_barrier(products.astype(jnp.bfloat16))
        summed = jnp.sum(rounded.astype(jnp.float32), axis=0)
        running = running.at[row_index].add(weight_col[:, None] * summed)
        return running, None

    start = jnp.zeros((blocks * (TOK_DEV + 1), D), jnp.float32)
    total, unused = lax.scan(one_expert, start, jnp.arange(EXPERTS, dtype=jnp.int32))
    total = total.reshape(blocks, TOK_DEV + 1, D)[:, :TOK_DEV, :].reshape(TOKENS, D)
    return total.astype(jnp.bfloat16)
```

```python
import functools

import jax
import jax.numpy as jnp
from jax import lax
from jax.experimental import pallas as pl
from jax.experimental.pallas import tpu as pltpu
from jax.sharding import PartitionSpec as P

SPAN = 2
LANES = 128
MESH = pl.DeviceIdType.MESH


def ring_stages(ring):
    return [(d, 2 * d == ring) for d in range(1, ring // 2 + 1)]


def copy_count(ring):
    stages = len(ring_stages(ring))
    exchange = 2 * (4 + 2 * stages) + 4 * 2 * stages + 4 * ring
    return 2 * exchange + 8 * ring + 8


def layer_kernel(
    ring,
    experts,
    tok_hbm,
    ids_ref,
    scores_ref,
    gate_hbm,
    up_hbm,
    down_hbm,
    out_ref,
    rows_in,
    gate,
    up,
    down,
    act,
    terms,
    twin_in,
    az_in,
    ap_in,
    bp_in,
    bz_in,
    send_sem,
    recv_sem,
    local_sem,
):
    tok, width = out_ref.shape
    half_rows = ring * 4 * tok
    me = lax.axis_index("expert")
    core, plane, level = me % 2, (me // 2) % 4, me // 8
    px = plane + 1 - 2 * (plane % 2)
    py = plane + 2 - 4 * (plane // 2)
    pd = 3 - plane

    def device(zz, pp, cc):
        return zz * 8 + pp * 2 + cc

    def lev(step):
        return (level + step + ring) % ring

    dev_x, dev_y = device(level, px, core), device(level, py, core)
    dev_up, dev_dn = device(lev(1), plane, core), device(lev(-1), plane, core)
    twin = device(level, plane, 1 - core)

    def rows(zz, pp, cc=core):
        return pl.ds(pl.multiple_of((cc * (4 * ring) + zz * 4 + pp) * tok, tok), tok)

    quarter = width // 4
    wide = width + rows_in.shape[1] - width
    a_all, a_sub = pl.ds(0, 2 * quarter), (pl.ds(0, quarter), pl.ds(quarter, quarter))
    b_all = pl.ds(2 * quarter, wide - 2 * quarter)
    b_sub = (pl.ds(2 * quarter, quarter), pl.ds(3 * quarter, wide - 3 * quarter))
    stages = ring_stages(ring)

    loads = [
        pltpu.make_async_copy(tok_hbm, rows_in.at[rows(level, plane), pl.ds(0, width)], local_sem.at[0]),
        pltpu.make_async_copy(gate_hbm.at[0], gate, local_sem.at[1]),
        pltpu.make_async_copy(up_hbm.at[0], up, local_sem.at[2]),
        pltpu.make_async_copy(down_hbm.at[0], down, local_sem.at[3]),
    ]
    for load in loads:
        load.start()

    scores = scores_ref[...]
    routed = 2.5 * scores / jnp.sum(scores, axis=1, keepdims=True)
    ids = ids_ref[...]
    spare = wide - width
    lane = lax.broadcasted_iota(jnp.int32, (tok, spare), 1)
    table = jnp.zeros((tok, spare), jnp.float32)
    for k in range(ids.shape[1]):
        hit = (lane == ids[:, k : k + 1]) | (lane == ids[:, k : k + 1] + experts)
        table = table + jnp.where(hit, routed[:, k : k + 1], 0.0)
    high = table.astype(jnp.bfloat16).astype(jnp.float32)
    table = jnp.where(lane < experts, high, table - high)
    rows_in[rows(level, plane), pl.ds(width, spare)] = table.astype(jnp.bfloat16)

    barrier = pltpu.get_barrier_semaphore()
    friends = [twin, dev_x, dev_y] + ([dev_up, dev_dn] if ring > 1 else [])
    for friend in friends:
        pl.semaphore_signal(barrier, inc=1, device_id={"expert": friend}, device_id_type=MESH)
    loads[0].wait()
    pl.semaphore_wait(barrier, len(friends))

    sent = []

    def send(src, dst, target):
        number = len(sent)
        copy = pltpu.make_async_remote_copy(
            src_ref=src,
            dst_ref=dst,
            send_sem=send_sem.at[number],
            recv_sem=recv_sem.at[number],
            device_id={"expert": target},
            device_id_type=MESH,
        )
        copy.start()
        sent.append(copy)
        return copy

    def spread(zz, pp, cols, target):
        piece = rows_in.at[rows(zz, pp), cols]
        return send(piece, piece, target)

    from_twin = []

    def share(zz, pp, cols):
        from_twin.append(spread(zz, pp, cols, twin))

    def ring_send(stage, way, pp, cols, sub):
        d, split = stages[stage]
        step = -(d - 1) if way == 0 else d - 1
        return spread(lev(step), pp, sub[way] if split else cols, dev_up if way == 0 else dev_dn)

    def ring_start(pp, cols, sub):
        return [ring_send(0, way, pp, cols, sub) for way in (0, 1)] if stages else []

    def ring_step(stage, copies, pp, cols, sub, landed):
        d, split = stages[stage]
        later = []
        for way in (0, 1):
            copies[way].wait_recv()
            if stage + 1 < len(stages):
                later.append(ring_send(stage + 1, way, pp, cols, sub))
            if not split:
                landed(lev(-d if way == 0 else d))
        if split:
            landed(lev(d))
        return later

    def plane_start(zz, cols):
        return [spread(zz, plane, cols, dev_x), spread(zz, plane, cols, dev_y)]

    def plane_step(copies, zz, sub, landed):
        copies[0].wait_recv()
        later = [spread(zz, px, sub[0], dev_y)]
        landed(px)
        copies[1].wait_recv()
        later.append(spread(zz, py, sub[1], dev_x))
        landed(py)
        return later

    b_ring = ring_start(plane, b_all, b_sub)
    a_plane = plane_start(level, a_all)
    a_flows, b_flows = [], []

    def a_landed(pp):
        a_flows.append((pp, ring_start(pp, a_all, a_sub)))
        share(level, pp, a_all)

    def b_landed(zz):
        b_flows.append((zz, plane_start(zz, b_all)))
        share(zz, plane, b_all)

    a_landed(plane)
    b_landed(level)
    a_plane = plane_step(a_plane, level, a_sub, a_landed)
    for stage in range(len(stages)):
        b_ring = ring_step(stage, b_ring, plane, b_all, b_sub, b_landed)
    for copy in a_plane:
        copy.wait_recv()
    a_landed(pd)
    span = max(len(a_flows), len(b_flows))
    for i in range(span):
        if i < len(a_flows) and stages:
            pp, copies = a_flows[i]
            copies = ring_step(0, copies, pp, a_all, a_sub, lambda zz, pp=pp: share(zz, pp, a_all))
            a_flows[i] = (pp, copies)
        if i < len(b_flows):
            zz, copies = b_flows[i]
            b_flows[i] = (
                zz,
                plane_step(copies, zz, b_sub, lambda pp, zz=zz: share(zz, pp, b_all)),
            )
    for stage in range(1, len(stages)):
        for i in range(len(a_flows)):
            pp, copies = a_flows[i]
            copies = ring_step(
                stage, copies, pp, a_all, a_sub, lambda zz, pp=pp: share(zz, pp, a_all)
            )
            a_flows[i] = (pp, copies)
    for zz, copies in b_flows:
        for copy in copies:
            copy.wait_recv()
        share(zz, pd, b_all)
    for load in loads[1:]:
        load.wait()

    def hidden_units(first):
        block = pl.ds(pl.multiple_of(first, tok), half_rows)
        gate_val = jnp.dot(rows_in[block, pl.ds(0, width)], gate[...], preferred_element_type=jnp.float32)
        up_val = jnp.dot(rows_in[block, pl.ds(0, width)], up[...], preferred_element_type=jnp.float32)
        act[block, :] = (jax.nn.silu(gate_val) * up_val).astype(jnp.bfloat16)

    def share_of(first):
        block = pl.ds(pl.multiple_of(first, tok), half_rows)
        entry = rows_in[block, pl.ds(width, spare)].astype(jnp.float32)
        place = lax.broadcasted_iota(jnp.int32, entry.shape, 1)
        mine = me // SPAN
        hit = (place == mine) | (place == mine + experts)
        return jnp.sum(jnp.where(hit, entry, 0.0), axis=1, keepdims=True)

    own_first, twin_first = core * half_rows, (1 - core) * half_rows
    hidden_units(own_first)
    for copy in from_twin:
        copy.wait_recv()
    hidden_units(twin_first)

    weight = share_of(twin_first)
    twin_block = pl.ds(pl.multiple_of(twin_first, tok), half_rows)
    own_block = pl.ds(pl.multiple_of(own_first, tok), half_rows)
    swaps = []
    for q in range(4):
        cols = pl.ds(q * quarter, quarter)
        piece = jnp.dot(act[twin_block, :], down[:, cols], preferred_element_type=jnp.float32)
        terms[twin_block, cols] = (weight * piece).astype(jnp.bfloat16)
        swaps.append(send(terms.at[twin_block, cols], twin_in.at[q], twin))
    weight = share_of(own_first)
    for q in range(4):
        cols = pl.ds(q * quarter, quarter)
        piece = jnp.dot(act[own_block, :], down[:, cols], preferred_element_type=jnp.float32)
        swaps[q].wait_recv()
        total = weight * piece + twin_in[q].astype(jnp.float32)
        terms[own_block, cols] = total.astype(jnp.bfloat16)

    c_all, c_sub = pl.ds(2 * quarter, 2 * quarter), tuple(pl.ds(i * quarter, quarter) for i in (2, 3))

    def add(zz, pp, cols, *arrived):
        block = terms[rows(zz, pp), cols].astype(jnp.float32)
        for piece in arrived:
            block = block + piece.astype(jnp.float32)
        terms[rows(zz, pp), cols] = block.astype(jnp.bfloat16)

    def local(cols, start):
        return pl.ds(cols.start - start, cols.size)

    def fold_send(stage, way, pp, cols, sub, inbox):
        d, split = stages[stage]
        part = sub[way] if split else cols
        return send(
            terms.at[rows(lev(d if way == 0 else -d), pp), part],
            inbox.at[way, stage, :, local(part, cols.start)],
            dev_up if way == 0 else dev_dn,
        )

    def fold_start(pp, cols, sub, inbox):
        return [fold_send(len(stages) - 1, way, pp, cols, sub, inbox) for way in (0, 1)] if stages else []

    def fold_down(copies, pp, cols, sub, inbox):
        for stage in range(len(stages) - 1, 0, -1):
            d, split = stages[stage]
            later = []
            for way in (0, 1):
                part = sub[way] if split else cols
                copies[way].wait_recv()
                add(lev(d - 1 if way == 0 else 1 - d), pp, part, inbox[way, stage, :, local(part, cols.start)])
                later.append(fold_send(stage - 1, way, pp, cols, sub, inbox))
            copies = later
        return copies

    def fold_last(copies, pp, cols, sub, inbox):
        if not stages:
            return
        for copy in copies:
            copy.wait_recv()
        if stages[0][1]:
            for way in (0, 1):
                add(level, pp, sub[way], inbox[way, 0, :, local(sub[way], cols.start)])
        else:
            add(level, pp, cols, inbox[0, 0], inbox[1, 0])

    def cross_start(zz, cols, sub, inbox):
        return [
            send(terms.at[rows(zz, pd), sub[i]], inbox.at[i, 0, :, local(sub[i], cols.start)], target)
            for i, target in ((0, dev_x), (1, dev_y))
        ]

    def cross_down(copies, zz, cols, sub, inbox):
        copies[0].wait_recv()
        add(zz, py, sub[0], inbox[0, 0, :, local(sub[0], cols.start)])
        to_y = send(terms.at[rows(zz, py), cols], inbox.at[1, 1], dev_y)
        copies[1].wait_recv()
        add(zz, px, sub[1], inbox[1, 0, :, local(sub[1], cols.start)])
        to_x = send(terms.at[rows(zz, px), cols], inbox.at[0, 1], dev_x)
        return [to_y, to_x]

    planes = [pd, px, py, plane]
    levels = []
    for d, split in reversed(stages):
        levels += [lev(d)] if split else [lev(d), lev(-d)]
    if ring % 2 == 1 and ring > 1 and not levels:
        levels = []
    levels.append(level)
    a_fold = [fold_start(planes[j], a_all, a_sub, az_in.at[j]) for j in range(4)]
    b_cross = [cross_start(levels[i], c_all, c_sub, bp_in.at[i]) for i in range(len(levels))]
    for i in range(max(4, len(levels))):
        if i < 4:
            a_fold[i] = fold_down(a_fold[i], planes[i], a_all, a_sub, az_in.at[i])
        if i < len(levels):
            b_cross[i] = cross_down(b_cross[i], levels[i], c_all, c_sub, bp_in.at[i])
    a_cross, b_fold = None, None
    for i in range(max(4, len(levels))):
        if i < 4:
            fold_last(a_fold[i], planes[i], a_all, a_sub, az_in.at[i])
            if i == 0:
                a_cross = cross_start(level, a_all, a_sub, ap_in)
        if i < len(levels):
            for copy in b_cross[i]:
                copy.wait_recv()
            add(levels[i], plane, c_all, bp_in[i, 0, 1], bp_in[i, 1, 1])
            if i == (0 if stages and stages[-1][1] else min(1, len(levels) - 1)):
                b_fold = fold_start(plane, c_all, c_sub, bz_in)
        if i == 2:
            a_cross = cross_down(a_cross, level, a_all, a_sub, ap_in)
    b_fold = fold_down(b_fold, plane, c_all, c_sub, bz_in)
    for copy in a_cross:
        copy.wait_recv()
    out_ref[:, a_all] = (
        terms[rows(level, plane), a_all].astype(jnp.float32)
        + ap_in[0, 1].astype(jnp.float32)
        + ap_in[1, 1].astype(jnp.float32)
    ).astype(jnp.bfloat16)
    fold_last(b_fold, plane, c_all, c_sub, bz_in)
    out_ref[:, c_all] = terms[rows(level, plane), c_all]
    for copy in sent:
        copy.wait_send()


def body(ring, tokens, expert_ids, router_scores, gate_weight, up_weight, down_weight):
    tok, width = tokens.shape
    hidden = gate_weight.shape[2]
    slots = lax.axis_size("expert")
    experts = slots // SPAN
    spare = -(-2 * experts // LANES) * LANES
    all_rows, half = slots * tok, width // 2
    depth = max(1, len(ring_stages(ring)))
    bf16 = jnp.bfloat16
    anywhere = pl.BlockSpec(memory_space=pl.ANY)
    vmem = pl.BlockSpec(memory_space=pltpu.VMEM)
    mixed = pl.pallas_call(
        functools.partial(layer_kernel, ring, experts),
        out_shape=jax.ShapeDtypeStruct((tok, width), bf16),
        in_specs=[anywhere, vmem, vmem, anywhere, anywhere, anywhere],
        out_specs=vmem,
        scratch_shapes=[
            pltpu.VMEM((all_rows, width + spare), bf16),
            pltpu.VMEM((width, hidden), bf16),
            pltpu.VMEM((width, hidden), bf16),
            pltpu.VMEM((hidden, width), bf16),
            pltpu.VMEM((all_rows, hidden), bf16),
            pltpu.VMEM((all_rows, width), bf16),
            pltpu.VMEM((4, all_rows // 2, width // 4), bf16),
            pltpu.VMEM((4, 2, depth, tok, half), bf16),
            pltpu.VMEM((2, 2, tok, half), bf16),
            pltpu.VMEM((ring, 2, 2, tok, half), bf16),
            pltpu.VMEM((2, depth, tok, half), bf16),
            pltpu.SemaphoreType.DMA((copy_count(ring),)),
            pltpu.SemaphoreType.DMA((copy_count(ring),)),
            pltpu.SemaphoreType.DMA((4,)),
        ],
        compiler_params=pltpu.CompilerParams(
            collective_id=0, has_side_effects=True, vmem_limit_bytes=60 << 20
        ),
    )(tokens, expert_ids, router_scores, gate_weight, up_weight, down_weight)
    if lax.axis_size("hidden") == 1:
        return mixed
    return lax.psum_scatter(mixed, "hidden", scatter_dimension=1, tiled=True)


def solution(mesh):
    return jax.shard_map(
        functools.partial(body, mesh.shape["expert"] // 8),
        mesh=mesh,
        in_specs=(
            P(("groups", "expert"), None),
            P(("groups", "expert"), None),
            P(("groups", "expert"), None),
            P("expert", None, "hidden"),
            P("expert", None, "hidden"),
            P("expert", "hidden", None),
        ),
        out_specs=P(("groups", "expert"), "hidden"),
        check_vma=False,
    )
```

```python
import functools

import jax
import jax.numpy as jnp
from jax import lax
from jax.experimental import pallas as pl
from jax.experimental.pallas import tpu as pltpu
from jax.sharding import PartitionSpec as P

SPAN = 2
LANES = 128
MESH = pl.DeviceIdType.MESH


def copy_count(ring):
    exchange = 8 * (ring - 1) + 4 + 2 * (ring - 1) + 4 * (2 * ring - 1)
    return 2 * exchange + 16 * ring + 8


def layer_kernel(
    ring,
    experts,
    tok_hbm,
    ids_ref,
    scores_ref,
    gate_hbm,
    up_hbm,
    down_hbm,
    out_ref,
    rows_in,
    gate,
    up,
    down,
    act,
    terms,
    twin_in,
    az_in,
    ap_in,
    bp_in,
    bz_in,
    send_sem,
    recv_sem,
    local_sem,
):
    tok, width = out_ref.shape
    half_rows = ring * 4 * tok
    me = lax.axis_index("expert")
    core, plane, level = me % 2, (me // 2) % 4, me // 8
    px = plane + 1 - 2 * (plane % 2)
    py = plane + 2 - 4 * (plane // 2)
    pd = 3 - plane

    def device(zz, pp, cc):
        return zz * 8 + pp * 2 + cc

    def lev(step):
        return (level + step + ring) % ring

    def inside(step):
        return (level + step >= 0) & (level + step < ring)

    dev_x, dev_y = device(level, px, core), device(level, py, core)
    ways = (1, -1)
    next_dev = [device(lev(way), plane, core) for way in ways]
    twin = device(level, plane, 1 - core)

    def rows(zz, pp, cc=core):
        return pl.ds(pl.multiple_of((cc * (4 * ring) + zz * 4 + pp) * tok, tok), tok)

    quarter = width // 4
    wide = rows_in.shape[1]
    edge = quarter + 3 * quarter // 2
    a_all, a_sub = pl.ds(0, quarter), (pl.ds(0, quarter // 2), pl.ds(quarter // 2, quarter // 2))
    b_all = pl.ds(quarter, wide - quarter)
    b_sub = (pl.ds(quarter, edge - quarter), pl.ds(edge, wide - edge))
    c_all = pl.ds(quarter, width - quarter)
    c_sub = (pl.ds(quarter, edge - quarter), pl.ds(edge, width - edge))

    loads = [
        pltpu.make_async_copy(tok_hbm, rows_in.at[rows(level, plane), pl.ds(0, width)], local_sem.at[0]),
        pltpu.make_async_copy(gate_hbm.at[0], gate, local_sem.at[1]),
        pltpu.make_async_copy(up_hbm.at[0], up, local_sem.at[2]),
        pltpu.make_async_copy(down_hbm.at[0], down, local_sem.at[3]),
    ]
    for load in loads:
        load.start()

    scores = scores_ref[...]
    routed = 2.5 * scores / jnp.sum(scores, axis=0, keepdims=True)
    ids = ids_ref[...]
    spare = wide - width
    entry = lax.broadcasted_iota(jnp.int32, (spare, tok), 0)
    table = jnp.zeros((spare, tok), jnp.float32)
    for k in range(ids.shape[0]):
        hit = (entry == ids[k : k + 1]) | (entry == ids[k : k + 1] + experts)
        table = table + jnp.where(hit, routed[k : k + 1], 0.0)
    high = table.astype(jnp.bfloat16).astype(jnp.float32)
    table = jnp.where(entry < experts, high, table - high)
    rows_in[rows(level, plane), pl.ds(width, spare)] = table.T.astype(jnp.bfloat16)

    barrier = pltpu.get_barrier_semaphore()
    def greet(friend):
        pl.semaphore_signal(barrier, inc=1, device_id={"expert": friend}, device_id_type=MESH)

    for friend in (twin, dev_x, dev_y):
        greet(friend)
    for way, friend in zip(ways, next_dev):
        pl.when(inside(way))(functools.partial(greet, friend))
    loads[0].wait()
    pl.semaphore_wait(barrier, 3 + sum(inside(way).astype(jnp.int32) for way in ways))

    sent = []

    def plan(src, dst, target, leaves=None):
        number = len(sent)
        copy = pltpu.make_async_remote_copy(
            src_ref=src,
            dst_ref=dst,
            send_sem=send_sem.at[number],
            recv_sem=recv_sem.at[number],
            device_id={"expert": target},
            device_id_type=MESH,
        )
        sent.append((copy, leaves))
        return copy

    def send(src, dst, target):
        copy = plan(src, dst, target)
        copy.start()
        return copy

    def spread(zz, pp, cols, target, leaves=None):
        piece = rows_in.at[rows(zz, pp), cols]
        return plan(piece, piece, target, leaves)

    from_twin = []

    def share(zz, pp, cols, there=None):
        copy = spread(zz, pp, cols, twin, there)
        from_twin.append((copy, there))
        return copy

    def line(pp, cols):
        return [
            [
                spread(lev(-way * (d - 1)), pp, cols, next_dev[i], inside(-way * (d - 1)) & inside(way))
                for i, way in enumerate(ways)
            ]
            for d in range(1, ring)
        ]

    def start_line(flow):
        for i, way in enumerate(ways):
            if flow:
                pl.when(inside(way))(flow[0][i].start)

    def step_line(flow, d, i, after):
        way = ways[i]

        @pl.when(inside(-way * d))
        def _():
            flow[d - 1][i].wait_recv()
            if d < ring - 1:
                pl.when(inside(way))(flow[d][i].start)
            for copy in after:
                copy.start()

    def cross(zz, cols, sub, there=None):
        return [
            spread(zz, plane, cols, dev_x, there),
            spread(zz, plane, cols, dev_y, there),
            spread(zz, px, sub[0], dev_y, there),
            spread(zz, py, sub[1], dev_x, there),
        ]

    b_line = line(plane, b_all)
    a_cross = cross(level, a_all, a_sub)
    a_lines = {name: line(pp, a_all) for name, pp in (("own", plane), ("x", px), ("y", py), ("d", pd))}
    a_place = {"own": plane, "x": px, "y": py, "d": pd}
    b_flows = []

    start_line(b_line)
    a_cross[0].start()
    a_cross[1].start()

    def open_cross(zz, there=None):
        copies = cross(zz, b_all, b_sub, there)
        b_flows.append((zz, there, copies))
        return [copies[0], copies[1], share(zz, plane, b_all, there)]

    for copy in open_cross(level):
        copy.start()
    start_line(a_lines["own"])
    share(level, plane, a_all).start()
    for i, name in enumerate(("x", "y")):
        a_cross[i].wait_recv()
        a_cross[2 + i].start()
        start_line(a_lines[name])
        share(level, a_place[name], a_all).start()
    for i, way in enumerate(ways):
        if ring > 1:
            step_line(b_line, 1, i, open_cross(lev(-way), inside(-way)))
    a_cross[2].wait_recv()
    a_cross[3].wait_recv()
    start_line(a_lines["d"])
    share(level, pd, a_all).start()

    def step_cross(flow):
        zz, there, copies = flow
        shares = [share(zz, px, b_all, there), share(zz, py, b_all, there)]

        def act():
            for i in (0, 1):
                copies[i].wait_recv()
                copies[2 + i].start()
                shares[i].start()

        act() if there is None else pl.when(there)(act)

    def end_cross(flow):
        zz, there, copies = flow
        last = share(zz, pd, b_all, there)

        def act():
            copies[2].wait_recv()
            copies[3].wait_recv()
            last.start()

        act() if there is None else pl.when(there)(act)

    def step_a(d):
        for name, flow in a_lines.items():
            for i, way in enumerate(ways):
                there = inside(-way * d)
                step_line(flow, d, i, [share(lev(-way * d), a_place[name], a_all, there)])

    step_cross(b_flows[0])
    for d in range(1, ring):
        if d + 1 < ring:
            for i, way in enumerate(ways):
                step_line(b_line, d + 1, i, open_cross(lev(-way * (d + 1)), inside(-way * (d + 1))))
        for flow in b_flows[max(0, 2 * d - 3) : 2 * d - 1]:
            end_cross(flow)
        step_cross(b_flows[2 * d - 1])
        step_cross(b_flows[2 * d])
        step_a(d)
    for flow in b_flows[max(0, 2 * ring - 3) :]:
        end_cross(flow)
    for load in loads[1:]:
        load.wait()

    def hidden_units(first):
        block = pl.ds(pl.multiple_of(first, tok), half_rows)
        gate_val = jnp.dot(rows_in[block, pl.ds(0, width)], gate[...], preferred_element_type=jnp.float32)
        up_val = jnp.dot(rows_in[block, pl.ds(0, width)], up[...], preferred_element_type=jnp.float32)
        act[block, :] = (jax.nn.silu(gate_val) * up_val).astype(jnp.bfloat16)

    def share_of(first):
        block = pl.ds(pl.multiple_of(first, tok), half_rows)
        entry = rows_in[block, pl.ds(width, spare)].astype(jnp.float32)
        place = lax.broadcasted_iota(jnp.int32, entry.shape, 1)
        mine = me // SPAN
        hit = (place == mine) | (place == mine + experts)
        return jnp.sum(jnp.where(hit, entry, 0.0), axis=1, keepdims=True)

    own_first, twin_first = core * half_rows, (1 - core) * half_rows
    hidden_units(own_first)
    for copy, there in from_twin:
        copy.wait_recv() if there is None else pl.when(there)(copy.wait_recv)
    hidden_units(twin_first)

    weight = share_of(twin_first)
    twin_block = pl.ds(pl.multiple_of(twin_first, tok), half_rows)
    own_block = pl.ds(pl.multiple_of(own_first, tok), half_rows)
    swaps = []
    for q in range(4):
        cols = pl.ds(q * quarter, quarter)
        piece = jnp.dot(act[twin_block, :], down[:, cols], preferred_element_type=jnp.float32)
        terms[twin_block, cols] = (weight * piece).astype(jnp.bfloat16)
        swaps.append(send(terms.at[twin_block, cols], twin_in.at[q], twin))
    weight = share_of(own_first)
    for q in range(4):
        cols = pl.ds(q * quarter, quarter)
        piece = jnp.dot(act[own_block, :], down[:, cols], preferred_element_type=jnp.float32)
        swaps[q].wait_recv()
        total = weight * piece + twin_in[q].astype(jnp.float32)
        terms[own_block, cols] = total.astype(jnp.bfloat16)

    def add(zz, pp, cols, *arrived):
        block = terms[rows(zz, pp), cols].astype(jnp.float32)
        for piece in arrived:
            block = block + piece.astype(jnp.float32)
        terms[rows(zz, pp), cols] = block.astype(jnp.bfloat16)

    def local(cols, start):
        return pl.ds(cols.start - start, cols.size)

    def fold(pp, cols, inbox):
        return [
            [
                plan(terms.at[rows(lev(way * d), pp), cols], inbox.at[i, d - 1], next_dev[i], inside(way * d))
                for i, way in enumerate(ways)
            ]
            for d in range(1, ring)
        ]

    def fold_start(flow):
        for i, way in enumerate(ways):
            if flow:
                pl.when(inside(way * (ring - 1)))(flow[-1][i].start)

    def fold_step(flow, d, pp, cols, inbox):
        for i, way in enumerate(ways):

            @pl.when(inside(-way) & inside(way * (d - 1)))
            def _():
                flow[d - 1][i].wait_recv()
                add(lev(way * (d - 1)), pp, cols, inbox[i, d - 1])

            if d > 1:
                pl.when(inside(way * (d - 1)))(flow[d - 2][i].start)

    def cross_start(zz, cols, sub, inbox):
        return [
            send(terms.at[rows(zz, pd), sub[i]], inbox.at[i, 0, :, local(sub[i], cols.start)], target)
            for i, target in ((0, dev_x), (1, dev_y))
        ]

    def cross_down(copies, zz, cols, sub, inbox):
        copies[0].wait_recv()
        add(zz, py, sub[0], inbox[0, 0, :, local(sub[0], cols.start)])
        to_y = send(terms.at[rows(zz, py), cols], inbox.at[1, 1], dev_y)
        copies[1].wait_recv()
        add(zz, px, sub[1], inbox[1, 0, :, local(sub[1], cols.start)])
        to_x = send(terms.at[rows(zz, px), cols], inbox.at[0, 1], dev_x)
        return [to_y, to_x]

    planes = [pd, px, py, plane]
    levels = [zz for i in range(ring // 2) for zz in (ring - 1 - i, i)] + [ring // 2] * (ring % 2)
    a_fold = [fold(pp, a_all, az_in.at[j]) for j, pp in enumerate(planes)]
    b_fold = fold(plane, c_all, bz_in)
    b_cross = [cross_start(zz, c_all, c_sub, bp_in.at[i]) for i, zz in enumerate(levels)]
    for flow in a_fold:
        fold_start(flow)

    def a_step(d, j):
        fold_step(a_fold[j], d, planes[j], a_all, az_in.at[j])

    def b_down(i):
        b_cross[i] = cross_down(b_cross[i], levels[i], c_all, c_sub, bp_in.at[i])

    def b_sum(i):
        for copy in b_cross[i]:
            copy.wait_recv()
        add(levels[i], plane, c_all, bp_in[i, 0, 1], bp_in[i, 1, 1])
        if i == min(1, ring - 1):
            fold_start(b_fold)

    b_work = []
    for i in range(ring):
        b_work.append(functools.partial(b_down, i))
        if i > 0:
            b_work.append(functools.partial(b_sum, i - 1))
    b_work.append(functools.partial(b_sum, ring - 1))
    a_work = [functools.partial(a_step, d, j) for d in range(ring - 1, 0, -1) for j in range(4)]
    for i in range(max(len(a_work), len(b_work))):
        if i * len(b_work) // len(a_work or b_work) != (i + 1) * len(b_work) // len(a_work or b_work):
            b_work[i * len(b_work) // len(a_work or b_work)]()
        if i < len(a_work):
            a_work[i]()
    a_cross = cross_start(level, a_all, a_sub, ap_in)
    a_cross = cross_down(a_cross, level, a_all, a_sub, ap_in)
    for d in range(ring - 1, 0, -1):
        fold_step(b_fold, d, plane, c_all, bz_in)
    for copy in a_cross:
        copy.wait_recv()
    add(level, plane, a_all, ap_in[0, 1], ap_in[1, 1])
    out_ref[...] = terms[rows(level, plane), :]
    for copy, leaves in sent:
        copy.wait_send() if leaves is None else pl.when(leaves)(copy.wait_send)


def body(ring, tokens, expert_ids, router_scores, gate_weight, up_weight, down_weight):
    tok, width = tokens.shape
    hidden = gate_weight.shape[2]
    slots = lax.axis_size("expert")
    experts = slots // SPAN
    spare = -(-2 * experts // LANES) * LANES
    all_rows, narrow, broad = slots * tok, width // 4, width - width // 4
    depth = max(1, ring - 1)
    bf16 = jnp.bfloat16
    anywhere = pl.BlockSpec(memory_space=pl.ANY)
    vmem = pl.BlockSpec(memory_space=pltpu.VMEM)
    mixed = pl.pallas_call(
        functools.partial(layer_kernel, ring, experts),
        out_shape=jax.ShapeDtypeStruct((tok, width), bf16),
        in_specs=[anywhere, vmem, vmem, anywhere, anywhere, anywhere],
        out_specs=vmem,
        scratch_shapes=[
            pltpu.VMEM((all_rows, width + spare), bf16),
            pltpu.VMEM((width, hidden), bf16),
            pltpu.VMEM((width, hidden), bf16),
            pltpu.VMEM((hidden, width), bf16),
            pltpu.VMEM((all_rows, hidden), bf16),
            pltpu.VMEM((all_rows, width), bf16),
            pltpu.VMEM((4, all_rows // 2, width // 4), bf16),
            pltpu.VMEM((4, 2, depth, tok, narrow), bf16),
            pltpu.VMEM((2, 2, tok, narrow), bf16),
            pltpu.VMEM((ring, 2, 2, tok, broad), bf16),
            pltpu.VMEM((2, depth, tok, broad), bf16),
            pltpu.SemaphoreType.DMA((copy_count(ring),)),
            pltpu.SemaphoreType.DMA((copy_count(ring),)),
            pltpu.SemaphoreType.DMA((4,)),
        ],
        compiler_params=pltpu.CompilerParams(
            collective_id=0, has_side_effects=True, vmem_limit_bytes=60 << 20
        ),
    )(tokens, expert_ids.T, router_scores.T, gate_weight, up_weight, down_weight)
    if lax.axis_size("hidden") == 1:
        return mixed
    return lax.psum_scatter(mixed, "hidden", scatter_dimension=1, tiled=True)


def solution(mesh):
    return jax.shard_map(
        functools.partial(body, mesh.shape["expert"] // 8),
        mesh=mesh,
        in_specs=(
            P(("groups", "expert"), None),
            P(("groups", "expert"), None),
            P(("groups", "expert"), None),
            P("expert", None, "hidden"),
            P("expert", None, "hidden"),
            P("expert", "hidden", None),
        ),
        out_specs=P(("groups", "expert"), "hidden"),
        check_vma=False,
    )
```
